512 devices in a mesh: gx: 16 (over y, core), gy: 8 (over z_hi, x), gz: 4 (over z_lo).
Axes of the slice: x: 4, y: 8, z: 8 (z_hi: 2, z_lo: 4; z = z_hi * 4 + z_lo), core: 2. Of those that a mesh axis runs over, the one named last changes fastest.
Arguments:
- positions: float32 [3, 16, 8, 4, 512], P(None, 'gx', 'gy', 'gz'), may hold values from 0 to 1
- velocities: float32 [3, 16, 8, 4, 512], P(None, 'gx', 'gy', 'gz'), may hold values from -6 to 6
- charges: float32 [16, 8, 4, 512], P('gx', 'gy', 'gz'), may hold values from -5 to 5
- cluster_atoms: int32 [16, 8, 4, 768], P('gx', 'gy', 'gz'), may hold values from 0 to 512, as said below
- pair_list: int32 [3, 16, 8, 4, 256], P(None, 'gx', 'gy', 'gz'), may hold values from 0 to 124, as said below
Outputs:
- new_positions: float32 [3, 16, 8, 4, 512], P(None, 'gx', 'gy', 'gz')
- new_velocities: float32 [3, 16, 8, 4, 512], P(None, 'gx', 'gy', 'gz')
- last_forces: float32 [3, 16, 8, 4, 512], P(None, 'gx', 'gy', 'gz')
The draws below stay inside these ranges and needn't reach their ends.
Inputs may be any that keep to these rules, and one draw needn't show every extreme that they name: `cluster_atoms`: on every domain each atom index below 512 stands in exactly one slot; all other slots hold 512, meaning empty. `pair_list`: row 0 and row 1 lie in 0 to 5, row 2 in 0 to 124; on every domain each of the 125 shift indices appears in at least 2 listed pairs.
All inputs are finite; a program needn't handle non-finite values.
Results may differ from the reference program's by a relative error of at most 0.0001.
Values sent between devices are 32-bit elements; how exact they have to be, the bound alone decides.
A program may use at most 64 MiB of HBM per device.

```python
import jax
import jax.numpy as jnp
from jax import lax

CLUSTER = 128
A_DEV = 512
CL_DEV = 6
PAIRS_DEV = 256
STEPS = 2
N_GX = 16
N_GY = 8
N_GZ = 4


def draw_cluster_atoms(key, part):
    device_count = N_GX * N_GY * N_GZ
    slot_count = CL_DEV * CLUSTER

    def per_device(device_key):
        shuffled = jax.random.permutation(device_key, jnp.arange(slot_count, dtype=jnp.int32))
        return jnp.minimum(shuffled, A_DEV).astype(jnp.int32)
    tables = jax.vmap(per_device)(jax.random.split(jax.random.fold_in(key, 11), device_count))
    return tables.reshape(N_GX, N_GY, N_GZ, slot_count)


def draw_pair_list(key, part):
    device_count = N_GX * N_GY * N_GZ
    pair_count = PAIRS_DEV
    covered = 125 * (pair_count // 125)

    def per_device(device_key):
        sub_keys = jax.random.split(device_key, 4)
        ordinal = jnp.arange(pair_count, dtype=jnp.int32)
        extra_shift = jax.random.randint(sub_keys[0], (pair_count,), 0, 125, dtype=jnp.int32)
        shift_index = jnp.where(ordinal < covered, ordinal % 125, extra_shift)
        shift_index = jax.random.permutation(sub_keys[1], shift_index)
        left_cluster = jax.random.randint(sub_keys[2], (pair_count,), 0, CL_DEV, dtype=jnp.int32)
        right_cluster = jax.random.randint(sub_keys[3], (pair_count,), 0, CL_DEV, dtype=jnp.int32)
        return jnp.stack([left_cluster, right_cluster, shift_index])
    pair_rows = jax.vmap(per_device)(jax.random.split(jax.random.fold_in(key, 23), device_count))
    return jnp.transpose(pair_rows, (1, 0, 2)).reshape(3, N_GX, N_GY, N_GZ, pair_count).astype(jnp.int32)


def block_levels(own_key, shape, cuts, smallest, largest):
    factor_of = 1.0
    for position, blocks in cuts:
        steps = jax.random.uniform(jax.random.fold_in(jax.random.fold_in(own_key, 6), position), (blocks,), jnp.float32, smallest / len(cuts), largest / len(cuts))
        factor_of = factor_of * jnp.repeat(jnp.exp(steps), shape[position] // blocks).reshape((-1,) + (1,) * (len(shape) - 1 - position))
    return factor_of


def noise(key, shape, spread, bound, pieces=(), held_as=jnp.bfloat16):
    values = jax.random.normal(key, shape, jnp.float32) * spread
    if len(pieces) > 0:
        values = block_levels(key, shape, pieces, -0.22, 0.18) * values
    return jnp.clip(values, min=-bound, max=bound).astype(held_as)


def setup_inputs(seed: int = 0) -> dict:
    splits = jax.random.split(jax.random.key(seed), 6)
    positions = jnp.clip(1.0 * jax.random.uniform(splits[0], (3, N_GX, N_GY, N_GZ, A_DEV), jnp.float32) ** block_levels(splits[0], (3, N_GX, N_GY, N_GZ, A_DEV), ((1, 16), (2, 8), (3, 4)), -0.2, 0.2), 0.0, 1.0)
    velocities = noise(splits[1], (3, N_GX, N_GY, N_GZ, A_DEV), 1.0, 6.0, ((1, 16), (2, 8), (3, 4)), jnp.float32)
    charges = noise(splits[2], (N_GX, N_GY, N_GZ, A_DEV), 1.0, 5.0, ((0, 16), (1, 8), (2, 4)), jnp.float32)
    cluster_atoms = draw_cluster_atoms(jax.random.fold_in(splits[5], 71), 0)
    pair_list = draw_pair_list(jax.random.fold_in(splits[5], 71), 0)
    return {"positions": positions, "velocities": velocities, "charges": charges, "cluster_atoms": cluster_atoms, "pair_list": pair_list}


CUTOFF_SQ = 4.0
SOFTENING = 0.5
TIME_STEP = 0.02


def pair_terms(left_xyz, left_charge, right_xyz, right_charge):
    separation = left_xyz[:, :, :, None] - right_xyz[:, :, None, :]
    distance_sq = jnp.sum(separation * separation, axis=0)
    window_term = jnp.maximum(1.0 - distance_sq / CUTOFF_SQ, 0.0)
    inverse = 1.0 / (distance_sq + SOFTENING)
    scalar = 2.0 * left_charge[:, :, None] * right_charge[:, None, :] * (
        3.0 * window_term * window_term * inverse / CUTOFF_SQ
        + window_term * window_term * window_term * inverse * inverse)
    pair_force = scalar[None] * separation
    return jnp.sum(pair_force, axis=3), -jnp.sum(pair_force, axis=2)


def forces_of(coords, atom_slots, slot_charge, left_rows, right_rows, offsets):
    device_count = atom_slots.shape[0]
    slot_count = atom_slots.shape[1]
    padded = jnp.concatenate([coords, jnp.zeros((3, device_count, 1), jnp.float32)], axis=2)
    slot_xyz = jnp.take_along_axis(padded, jnp.broadcast_to(atom_slots[None], (3, device_count, slot_count)), axis=2)
    slot_xyz = slot_xyz.reshape(3, device_count * CL_DEV, CLUSTER)
    block_size = 64
    blocks = left_rows.shape[0] // block_size

    def accumulate(carried, block_data):
        rows_left, rows_right, shift_vec = block_data
        left_xyz = slot_xyz[:, rows_left]
        right_xyz = slot_xyz[:, rows_right] + shift_vec[:, :, None]
        left_force, right_force = pair_terms(left_xyz, slot_charge[rows_left], right_xyz, slot_charge[rows_right])
        carried = carried.at[:, rows_left].add(left_force).at[:, rows_right].add(right_force)
        return carried, None

    start = jnp.zeros((3, device_count * CL_DEV, CLUSTER), jnp.float32)
    summed, _ = lax.scan(accumulate, start, (left_rows.reshape(blocks, block_size), right_rows.reshape(blocks, block_size), jnp.transpose(offsets.reshape(3, blocks, block_size), (1, 0, 2))))
    summed = summed.reshape(3, device_count, slot_count)

    def to_atoms(slot_force, slot_index):
        return jnp.zeros((3, A_DEV + 1), jnp.float32).at[:, slot_index].add(slot_force)[:, :A_DEV]

    return jax.vmap(to_atoms, in_axes=(1, 0), out_axes=1)(summed, atom_slots)


def reference(positions, velocities, charges, cluster_atoms, pair_list):
    device_count = N_GX * N_GY * N_GZ
    slot_count = CL_DEV * CLUSTER
    atom_slots = cluster_atoms.reshape(device_count, slot_count).astype(jnp.int32)
    charge_pad = jnp.concatenate([charges.reshape(device_count, A_DEV), jnp.zeros((device_count, 1), jnp.float32)], axis=1)
    slot_charge = jnp.take_along_axis(charge_pad, atom_slots, axis=1).reshape(device_count * CL_DEV, CLUSTER)
    pairs = pair_list.reshape(3, device_count, PAIRS_DEV).astype(jnp.int32)
    device = jnp.arange(device_count, dtype=jnp.int32)[:, None]
    cell_x = device // (N_GY * N_GZ)
    cell_y = (device // N_GZ) % N_GY
    cell_z = device % N_GZ
    shift_index = pairs[2]
    delta_x = shift_index // 25 - 2
    delta_y = (shift_index // 5) % 5 - 2
    delta_z = shift_index % 5 - 2
    source = (((cell_x + delta_x) % N_GX) * N_GY + (cell_y + delta_y) % N_GY) * N_GZ + (cell_z + delta_z) % N_GZ
    left_rows = (device * CL_DEV + pairs[0]).reshape(-1).astype(jnp.int32)
    right_rows = (source * CL_DEV + pairs[1]).reshape(-1).astype(jnp.int32)
    offsets = jnp.stack([delta_x, delta_y, delta_z]).reshape(3, -1).astype(jnp.float32)
    coords = positions.reshape(3, device_count, A_DEV)
    velocity = velocities.reshape(3, device_count, A_DEV)
    forces = jnp.zeros_like(coords)
    for step_index in range(STEPS):
        forces = forces_of(coords, atom_slots, slot_charge, left_rows, right_rows, offsets)
        velocity = velocity + TIME_STEP * forces
        coords = coords + TIME_STEP * velocity
    return coords.reshape(positions.shape), velocity.reshape(positions.shape), forces.reshape(positions.shape)
```

```python
import functools

import jax
import jax.numpy as jnp
from jax import lax
from jax.experimental import pallas as pl
from jax.experimental.pallas import tpu as pltpu
from jax.sharding import PartitionSpec as P

f32, bf16, i32 = jnp.float32, jnp.bfloat16, jnp.int32
MESH = pl.DeviceIdType.MESH
AXES = ("gx", "gy", "gz")
CLUSTER = 128
CLUSTERS = 6
ATOMS = 512
STEPS = 2
TIME_STEP = 0.02
NB = 10
KR = 32
SR = 48
SLOTS = 384
PLACE = (2, 3, 0, 1, 2)
SIDE = (0, 1, 3, 4)


def split2(v):
    hi = v.astype(bf16).astype(f32)
    return hi, v - hi

def split3f(v):
    a = v.astype(bf16).astype(f32)
    r = v - a
    b = r.astype(bf16).astype(f32)
    return a, b, r - b

def shifted(block, shift):
    return [block[c] + shift[c] if shift[c] is not None else block[c] for c in range(3)]

def weight_rows(coords, charge):
    q = 0.125 * charge
    parts = [split2(q * c) for c in coords] + [split2(q)]
    return [a for a, _ in parts] + [b for _, b in parts]

def put_rows(t_ref, rows, base):
    for n, r in enumerate(rows):
        t_ref[pl.ds(base + n, 8, stride=SR), :] = r

def build_v(t_ref, v_ref, wv_ref, coords, charge, base):
    half = [0.5 * c for c in coords]
    rows = []
    for h in half:
        a, b, c = split3f(h)
        rows += [a, b, a, b, c, a]
    rows += list(split3f(-(half[0]*half[0] + half[1]*half[1] + half[2]*half[2])))
    one = jnp.ones_like(charge)
    rows += [one, one, one]
    put_rows(t_ref, rows, 0)
    put_rows(t_ref, weight_rows(coords, charge), KR)
    for k in range(6):
        v_ref[base + k] = t_ref[k*SR:k*SR+KR, :].astype(bf16)
        wv_ref[base + k] = t_ref[k*SR+KR:(k+1)*SR, :].astype(bf16)

def build_u(t_ref, u_ref, wu_ref, coords, charge, base):
    half = [0.5 * c for c in coords]
    rows = []
    for h in half:
        a, b, c = split3f(h)
        a, b, c = 2.0*a, 2.0*b, 2.0*c
        rows += [a, a, b, b, a, c]
    one = jnp.ones_like(charge)
    rows += [one, one, one]
    rows += list(split3f(1.0 - (half[0]*half[0] + half[1]*half[1] + half[2]*half[2])))
    put_rows(t_ref, rows, 0)
    put_rows(t_ref, weight_rows(coords, charge), KR)
    for k in range(6):
        u_ref[base + k] = jnp.transpose(t_ref[k*SR:k*SR+KR, :]).astype(bf16)
        wu_ref[base + k] = t_ref[k*SR+KR:(k+1)*SR, :].astype(bf16)

def pair_block(code_ref, u_ref, v_ref, wu_ref, wv_ref, f_ref, rawl_ref, rawr_ref):
    def idx(n):
        ui, vi = code_ref[n >> 7, n & 127], code_ref[3 + (n >> 7), n & 127]
        return jnp.clip(ui, 0, u_ref.shape[0] - 1), jnp.clip(vi, 0, v_ref.shape[0] - 1)

    def geometry(slot, n):
        ui, vi = idx(n)
        g0 = jnp.dot(u_ref[ui], v_ref[vi], preferred_element_type=f32)
        g = jnp.maximum(g0, 0.0)
        den = 1.125 - g0
        s = pl.reciprocal(den, approx=True)
        t = (g * s) * (2.0 - den * s)
        f = (g * t) * (t + 3.0)
        hi = f.astype(bf16)
        f_ref[slot, :, 0:128] = hi
        f_ref[slot, :, 128:256] = (f - hi.astype(f32)).astype(bf16)

    def sums(slot, n):
        ui, vi = idx(n)
        fv = f_ref[slot]
        wv = wv_ref[vi]
        left = lax.dot_general(jnp.concatenate([wv, wv], axis=1), fv, (((1,), (1,)), ((), ())),
                               preferred_element_type=f32)
        right = jnp.dot(wu_ref[ui], fv, preferred_element_type=f32)
        return left[0:8], right[0:8, 0:128] + right[0:8, 128:256]

    def keep(n, lr):
        rawl_ref[pl.ds(n, 8, stride=SLOTS), :] = lr[0]
        rawr_ref[pl.ds(n, 8, stride=SLOTS), :] = lr[1]

    return geometry, sums, keep

def block_start(b):
    return (b // 5) * 64 + (b % 5) * 10

def all_pairs(geometry, sums, keep):
    for n in range(NB):
        geometry(n, block_start(0) + n)

    def step(prev, now):
        found = []
        for n in range(NB):
            found.append(sums(n, prev(n)))
            geometry(n, now(n))
            if n > 1:
                keep(prev(n - 2), found[n - 2])
        keep(prev(NB - 2), found[NB - 2])
        keep(prev(NB - 1), found[NB - 1])

    def at(b):
        def f(n):
            e = jnp.maximum((b - 25) * NB + n, 0)
            return jnp.where(b < 25, block_start(jnp.minimum(b, 24)) + n, (e // 6) * 64 + 50 + e % 6)
        return f

    def body(b, c):
        step(at(b - 1), at(b))
        return c
    lax.fori_loop(1, 28, body, 0)
    last = at(27)
    for n in range(NB):
        keep(last(n), sums(n, last(n)))

def reduced(raw_ref, hot_ref):
    cols_hi, cols_lo = [], []
    for c in range(4):
        v = raw_ref[c*SLOTS:(c+1)*SLOTS, :] + raw_ref[(c+4)*SLOTS:(c+5)*SLOTS, :]
        hi = v.astype(bf16)
        cols_hi.append(hi)
        cols_lo.append((v - hi.astype(f32)).astype(bf16))
    rhs = jnp.concatenate([jnp.concatenate(cols_hi, axis=1), jnp.concatenate(cols_lo, axis=1)], axis=0)
    return jnp.dot(hot_ref[...], rhs, preferred_element_type=f32)

def make_hot(code_rows, rows):
    out = []
    for r in code_rows:
        it = lax.broadcasted_iota(i32, (rows, 128), 0)
        out.append(jnp.where(it == r, 1.0, 0.0).astype(bf16))
    one = jnp.concatenate(out, axis=1)
    return jnp.concatenate([one, one], axis=1)


def tables(plate, tower, t_ref, u_ref, v_ref, wu_ref, wv_ref):
    for q in range(5):
        blk = tower(q)
        sh = (None, float(2 - q) if q != 2 else None, None)
        build_u(t_ref, u_ref, wu_ref, shifted(blk, sh), blk[3], q * 6)
    for p in range(5):
        for r in range(5):
            blk = plate(p, PLACE[r])
            sh = (float(p - 2) if p != 2 else None, None, float(r - 2) if r != 2 else None)
            build_v(t_ref, v_ref, wv_ref, shifted(blk, sh), blk[3], (p * 5 + r) * 6)

def finish(plate, tower, out_r, out_l, fr_ref, fl_ref):
    for p in range(5):
        held = {}
        for r in range(5):
            blk = plate(p, PLACE[r])
            sh = (float(p - 2) if p != 2 else None, None, float(r - 2) if r != 2 else None)
            x = shifted(blk, sh)
            rows = slice((p*5+r)*8, (p*5+r)*8+8)
            s = out_r[rows, 384:512]
            fc = [blk[3] * (x[c] * s - out_r[rows, c*128:(c+1)*128]) for c in range(3)]
            z = PLACE[r]
            held[z] = fc if z not in held else [a + b for a, b in zip(held[z], fc)]
        for z in range(4):
            for c in range(3):
                fr_ref[p, z, c] = held[z][c]
    for q in range(5):
        blk = tower(q)
        sh = (None, float(2 - q) if q != 2 else None, None)
        x = shifted(blk, sh)
        s = out_l[q*8:q*8+8, 384:512]
        for c in range(3):
            fl_ref[q, c] = blk[3] * (x[c] * s - out_l[q*8:q*8+8, c*128:(c+1)*128])


def split3(value):
    hi = value.astype(bf16)
    rest = value - hi.astype(f32)
    mid = rest.astype(bf16)
    lo = (rest - mid.astype(f32)).astype(bf16)
    return hi, mid, lo


def one_hot(atoms_ref):
    slots = atoms_ref.shape[1]
    rows = lax.broadcasted_iota(i32, (ATOMS, slots), 0)
    return jnp.where(rows == atoms_ref[...], 1.0, 0.0).astype(bf16)


def sort_pairs(pairs_ref, code_ref):
    count = pairs_ref.shape[2]
    left, right, t = pairs_ref[0], pairs_ref[1], pairs_ref[2]
    t25 = (t * 5243) >> 17
    t5 = (t * 205) >> 10
    q_row = (t5 - 5 * t25).astype(f32)
    pr_row = (t25 * 5 + t - 5 * t5).astype(f32)
    t_row = t.astype(f32)
    rows = jnp.concatenate([t_row, q_row, pr_row, jnp.zeros((125, count), f32)], axis=0)
    cols = jnp.concatenate(
        [jnp.transpose(rows[:, h * 128:(h + 1) * 128]) for h in range(count // 128)], axis=0)
    t_col, q_col, pr_col = cols[:, 0:1], cols[:, 1:2], cols[:, 2:3]
    a = lax.broadcasted_iota(i32, (count, count), 0)
    b = lax.broadcasted_iota(i32, (count, count), 1)
    same = jnp.where(t_col == t_row, 1.0, 0.0)
    earlier = jnp.where(b < a, 1.0, 0.0)
    rank_row = jnp.sum(same * jnp.where(a < b, 1.0, 0.0), axis=0, keepdims=True)
    rank_col = jnp.sum(same * earlier, axis=1, keepdims=True)
    extra_row = jnp.where(rank_row > 1.5, 1.0, 0.0)
    extra_col = jnp.sum(jnp.where(q_col == q_row, earlier * extra_row, 0.0), axis=1, keepdims=True)
    odd = jnp.where((q_col == 1.0) | (q_col == 3.0), 64.0, 0.0)
    place = jnp.where(rank_col < 1.5, 2.0 * pr_col + rank_col, 50.0 + extra_col)
    place = place + odd + 128.0 * q_col
    lane = lax.broadcasted_iota(i32, (count, 640), 1).astype(f32)
    hot = jnp.where(place == lane, 1.0, 0.0).astype(bf16)
    values = jnp.concatenate(
        [left.astype(f32) + 1.0, right.astype(f32) + 1.0, pr_row, jnp.zeros((13, count), f32)],
        axis=0).astype(bf16)
    out = jnp.dot(values, hot, preferred_element_type=f32)
    for q in range(5):
        code_ref[q] = out[0:8, q * 128:(q + 1) * 128].astype(i32)


def decode(blocks, code_vec_ref):
    left_rows, right_rows = [], []
    high = lax.broadcasted_iota(i32, (1, 128), 1) >= 64
    for h in range(3):
        blk = blocks(2 * h)
        if h < 2:
            blk = blk + blocks(2 * h + 1)
        i, j, pr = blk[0:1] - 1, blk[1:2] - 1, blk[2:3]
        q = 2 * h + (jnp.where(high, 1, 0) if h < 2 else jnp.zeros((1, 128), i32))
        code_vec_ref[h:h + 1, :] = q * CLUSTERS + jnp.maximum(i, 0)
        code_vec_ref[3 + h:4 + h, :] = pr * CLUSTERS + jnp.maximum(j, 0)
        left_rows.append(jnp.where(i < 0, -1, q * 8 + i))
        right_rows.append(jnp.where(j < 0, -1, pr * 8 + j))
    code_vec_ref[6:8, :] = jnp.zeros((2, 128), i32)
    return left_rows, right_rows


def kernel(sizes, pairs_ref, x_in, v_in, q_in, atoms_ref, x_out, v_out, f_out,
           plate_ref, tower_ref, vel_ref, fr_ref, fl_ref, landx_ref, landt_ref, landz_ref,
           zsum_ref, code_out_ref, code_in_ref, code_vec_ref, code_ref, slot_ref,
           t_ref, u_ref, v_ref, wu_ref, wv_ref, f_ref, rawl_ref, rawr_ref, hr_ref, hl_ref,
           local_sem, send_sem, recv_sem):
    me = tuple(lax.axis_index(axis) for axis in AXES)

    def peer(axis, offset):
        n = sizes[axis]
        ids = list(me)
        ids[axis] = lax.rem(me[axis] + (offset + n), n)
        return tuple(ids)

    barrier = pltpu.get_barrier_semaphore()
    partners = [(0, d) for d in (-2, -1, 1, 2)] + [(1, d) for d in (-2, -1, 1, 2)]
    partners += [(2, d) for d in (1, 2, 3)]
    for axis, d in partners:
        pl.semaphore_signal(barrier, 1, device_id=peer(axis, d), device_id_type=MESH)

    def copy(step, k, src, dst, to):
        return pltpu.make_async_remote_copy(
            src_ref=src, dst_ref=dst, send_sem=send_sem.at[step, k],
            recv_sem=recv_sem.at[step, k], device_id=to, device_id_type=MESH)

    def comps(step):
        return pl.ds(0, 4) if step == 0 else pl.ds(0, 3)

    def share_z(step, z):
        return copy(step, z - 1, plate_ref.at[step, 2, 0, comps(step)],
                    plate_ref.at[step, 2, z, comps(step)], peer(2, 4 - z))

    def share_t(step, q):
        return copy(step, 3 + SIDE.index(q), plate_ref.at[step, 2, 0, comps(step)],
                    tower_ref.at[step, q, comps(step)], peer(1, q - 2))

    def share_p(step, p, z):
        return copy(step, 7 + SIDE.index(p) * 4 + z, plate_ref.at[step, 2, z, comps(step)],
                    plate_ref.at[step, p, z, comps(step)], peer(0, 2 - p))

    def give_x(step, p):
        return copy(step, 23 + SIDE.index(p), fr_ref.at[step, p], landx_ref.at[step, p],
                    peer(0, p - 2))

    def give_t(step, q):
        return copy(step, 27 + SIDE.index(q), fl_ref.at[step, q], landt_ref.at[step, q],
                    peer(1, 2 - q))

    def give_z(step, z):
        return copy(step, 30 + z, zsum_ref.at[step, z], landz_ref.at[step, z], peer(2, z))

    def share_code(q):
        return copy(0, 34 + SIDE.index(q), code_out_ref.at[q], code_in_ref.at[q], peer(1, q - 2))

    data = jnp.concatenate(
        [x_in[c] for c in range(3)] + [q_in[...]] + [v_in[c] for c in range(3)]
        + [jnp.zeros((1, ATOMS), f32)], axis=0)
    hi, mid, lo = split3(data)
    stacked = jnp.concatenate([hi, mid, lo, jnp.zeros_like(hi)], axis=0)
    out = jnp.dot(stacked, one_hot(atoms_ref), preferred_element_type=f32)
    slot = out[0:8] + out[8:16] + out[16:24]
    vel_ref[...] = jnp.zeros_like(vel_ref)
    plate_ref[0, 2, 0] = jnp.zeros((4, 8, 128), f32)
    for k in range(CLUSTERS):
        lanes = slice(k * CLUSTER, (k + 1) * CLUSTER)
        for c in range(4):
            plate_ref[0, 2, 0, c, pl.ds(k, 1), :] = slot[c:c + 1, lanes]
        for c in range(3):
            vel_ref[c, pl.ds(k, 1), :] = slot[4 + c:5 + c, lanes]
    pl.semaphore_wait(barrier, len(partners))

    def start_share(step):
        for z in (2, 1, 3):
            share_z(step, z).start()
        for q in (0, 4, 1, 3):
            share_t(step, q).start()
        for p in SIDE:
            share_p(step, p, 0).start()

    def forward(step):
        for z in (1, 3, 2):
            share_z(step, z).wait_recv()
            for p in SIDE:
                share_p(step, p, z).start()

    def end_share(step):
        for q in SIDE:
            share_t(step, q).wait_recv()
        for z in (0, 1, 3, 2):
            for p in SIDE:
                share_p(step, p, z).wait_recv()

    start_share(0)
    sort_pairs(pairs_ref, code_out_ref)
    for q in SIDE:
        share_code(q).start()
    rawl_ref[...] = jnp.zeros_like(rawl_ref)
    rawr_ref[...] = jnp.zeros_like(rawr_ref)
    t_ref[...] = jnp.zeros_like(t_ref)
    forward(0)
    for q in SIDE:
        share_code(q).wait_recv()
    left_rows, right_rows = decode(
        lambda q: code_out_ref[q] if q == 2 else code_in_ref[q], code_vec_ref)
    to_smem = pltpu.make_async_copy(code_vec_ref, code_ref, local_sem)
    to_smem.start()
    hl_ref[...] = make_hot(left_rows, 40)
    hr_ref[...] = make_hot(right_rows, 200)
    to_smem.wait()

    geometry, sums, keep = pair_block(
        code_ref, u_ref, v_ref, wu_ref, wv_ref, f_ref, rawl_ref, rawr_ref)

    for step in range(STEPS):
        def plate(p, z):
            return ([plate_ref[step, p, z, c] for c in range(3)] + [plate_ref[0, p, z, 3]])

        def tower(q):
            if q == 2:
                return plate(2, 0)
            return [tower_ref[step, q, c] for c in range(3)] + [tower_ref[0, q, 3]]

        if step > 0:
            forward(step)
        end_share(step)
        tables(plate, tower, t_ref, u_ref, v_ref, wu_ref, wv_ref)
        all_pairs(geometry, sums, keep)
        out_r = reduced(rawr_ref, hr_ref)
        out_l = reduced(rawl_ref, hl_ref)
        finish(plate, tower, out_r, out_l, fr_ref.at[step], fl_ref.at[step])
        for p in SIDE:
            give_x(step, p).start()
        for q in SIDE:
            give_t(step, q).start()
        total = [[fr_ref[step, 2, z, c] for c in range(3)] for z in range(4)]
        for p in SIDE:
            give_x(step, p).wait_recv()
            for z in range(4):
                total[z] = [total[z][c] + landx_ref[step, p, z, c] for c in range(3)]
        for z in (2, 1, 3):
            for c in range(3):
                zsum_ref[step, z, c] = total[z][c]
            give_z(step, z).start()
        force = [total[0][c] + fl_ref[step, 2, c] for c in range(3)]
        for q in SIDE:
            give_t(step, q).wait_recv()
            force = [force[c] + landt_ref[step, q, c] for c in range(3)]
        for z in (1, 3, 2):
            give_z(step, z).wait_recv()
            force = [force[c] + landz_ref[step, z, c] for c in range(3)]
        velocity = [vel_ref[c] + TIME_STEP * force[c] for c in range(3)]
        coords = [plate_ref[step, 2, 0, c] + TIME_STEP * velocity[c] for c in range(3)]
        if step < STEPS - 1:
            for c in range(3):
                plate_ref[step + 1, 2, 0, c] = coords[c]
            start_share(step + 1)
            for c in range(3):
                vel_ref[c] = velocity[c]

    slot_ref[...] = jnp.zeros_like(slot_ref)
    for k in range(CLUSTERS):
        lanes = slice(k * CLUSTER, (k + 1) * CLUSTER)
        for c in range(3):
            slot_ref[pl.ds(c, 1), lanes] = coords[c][k:k + 1]
            slot_ref[pl.ds(3 + c, 1), lanes] = velocity[c][k:k + 1]
            slot_ref[pl.ds(6 + c, 1), lanes] = force[c][k:k + 1]
    stacked = jnp.concatenate(split3(slot_ref[...]), axis=0)
    out = lax.dot_general(
        stacked, one_hot(atoms_ref), (((1,), (1,)), ((), ())), preferred_element_type=f32)
    atom = out[0:16] + out[16:32] + out[32:48]
    for c in range(3):
        x_out[c] = atom[c:c + 1]
        v_out[c] = atom[3 + c:4 + c]
        f_out[c] = atom[6 + c:7 + c]

    for step in range(STEPS):
        for z in (1, 2, 3):
            share_z(step, z).wait_send()
            give_z(step, z).wait_send()
        for s in SIDE:
            share_t(step, s).wait_send()
            give_x(step, s).wait_send()
            give_t(step, s).wait_send()
            for z in range(4):
                share_p(step, s, z).wait_send()
    for q in SIDE:
        share_code(q).wait_send()


def shards(sizes, positions, velocities, charges, cluster_atoms, pair_list):
    slots = cluster_atoms.shape[-1]
    x = positions.reshape(3, 1, ATOMS)
    v = velocities.reshape(3, 1, ATOMS)
    q = charges.reshape(1, ATOMS)
    atoms = cluster_atoms.reshape(1, slots)
    pairs = pair_list.reshape(3, 1, pair_list.shape[-1])
    shape = jax.ShapeDtypeStruct((3, 1, ATOMS), f32)
    vmem = pl.BlockSpec(memory_space=pltpu.VMEM)
    outs = pl.pallas_call(
        functools.partial(kernel, sizes),
        out_shape=(shape, shape, shape),
        in_specs=[vmem] * 5,
        out_specs=(vmem, vmem, vmem),
        scratch_shapes=[
            pltpu.VMEM((STEPS, 5, 4, 4, 8, 128), f32),
            pltpu.VMEM((STEPS, 5, 4, 8, 128), f32),
            pltpu.VMEM((3, 8, 128), f32),
            pltpu.VMEM((STEPS, 5, 4, 3, 8, 128), f32),
            pltpu.VMEM((STEPS, 5, 3, 8, 128), f32),
            pltpu.VMEM((STEPS, 5, 4, 3, 8, 128), f32),
            pltpu.VMEM((STEPS, 5, 3, 8, 128), f32),
            pltpu.VMEM((STEPS, 4, 3, 8, 128), f32),
            pltpu.VMEM((STEPS, 4, 3, 8, 128), f32),
            pltpu.VMEM((5, 8, 128), i32),
            pltpu.VMEM((5, 8, 128), i32),
            pltpu.VMEM((8, 128), i32),
            pltpu.SMEM((8, 128), i32),
            pltpu.VMEM((16, slots), f32),
            pltpu.VMEM((9 * SR, 128), f32),
            pltpu.VMEM((30, 128, KR), bf16),
            pltpu.VMEM((150, KR, 128), bf16),
            pltpu.VMEM((30, 16, 128), bf16),
            pltpu.VMEM((150, 16, 128), bf16),
            pltpu.VMEM((NB, 128, 256), bf16),
            pltpu.VMEM((9 * SLOTS, 128), f32),
            pltpu.VMEM((9 * SLOTS, 128), f32),
            pltpu.VMEM((200, 2 * SLOTS), bf16),
            pltpu.VMEM((40, 2 * SLOTS), bf16),
            pltpu.SemaphoreType.DMA,
            pltpu.SemaphoreType.DMA((STEPS, 38)),
            pltpu.SemaphoreType.DMA((STEPS, 38)),
        ],
        compiler_params=pltpu.CompilerParams(collective_id=0, has_side_effects=True),
        name="leapfrog",
    )(pairs, x, v, q, atoms)
    return tuple(out.reshape(positions.shape) for out in outs)


def solution(mesh):
    spec3 = P(None, "gx", "gy", "gz", None)
    spec1 = P("gx", "gy", "gz", None)
    sizes = tuple(mesh.shape[axis] for axis in AXES)
    return jax.shard_map(
        functools.partial(shards, sizes),
        mesh=mesh,
        in_specs=(spec3, spec3, spec1, spec1, spec3),
        out_specs=(spec3, spec3, spec3),
        check_vma=False,
    )
```

```python
import functools

import jax
import jax.numpy as jnp
from jax import lax
from jax.experimental import pallas as pl
from jax.experimental.pallas import tpu as pltpu
from jax.sharding import PartitionSpec as P

f32, bf16, i32 = jnp.float32, jnp.bfloat16, jnp.int32
MESH = pl.DeviceIdType.MESH
AXES = ("gx", "gy", "gz")
CLUSTER = 128
CLUSTERS = 6
ATOMS = 512
STEPS = 2
TIME_STEP = 0.02
NB = 8
KR = 32
SR = 48
SLOTS = 384
PLACE = (2, 3, 0, 1, 2)
SIDE = (0, 1, 3, 4)
POSITIONS = (0, 1, 2, 0, 1, 2, 0, 1, 2, 0, 1, 2, 0, 1, 2, 3, 3, 3, 3, 3, 4, 4, 4, 4, 4, 0, 1, 2, 3, 4, 3, 4, 0, 1, 2)
GROUPS = (0, 0, 0, 2, 2, 2, 3, 3, 3, 4, 4, 4, 5, 5, 5, 0, 2, 3, 4, 5, 0, 2, 3, 4, 5, 6, 6, 6, 6, 6, 1, 1, 1, 1, 1)


def split2(v):
    hi = v.astype(bf16).astype(f32)
    return hi, v - hi


def split3f(v):
    a = v.astype(bf16).astype(f32)
    r = v - a
    b = r.astype(bf16).astype(f32)
    return a, b, r - b


def weight_rows(coords, charge):
    q = 0.125 * charge
    parts = [split2(q * c) for c in coords] + [split2(q)]
    return [a for a, _ in parts] + [b for _, b in parts]


def put_rows(t_ref, rows, base):
    for n, r in enumerate(rows):
        t_ref[pl.ds(base + n, 8, stride=SR), :] = r


def half_square(half):
    return half[0] * half[0] + half[1] * half[1] + half[2] * half[2]


def build_v(t_ref, v_ref, wv_ref, coords, charge, base):
    half = [0.5 * c for c in coords]
    rows = []
    for h in half:
        a, b, c = split3f(h)
        rows += [a, b, a, b, c, a]
    rows += list(split3f(-half_square(half)))
    one = jnp.ones_like(charge)
    rows += [one, one, one]
    put_rows(t_ref, rows, 0)
    put_rows(t_ref, weight_rows(coords, charge), KR + 8)
    for k in range(CLUSTERS):
        v_ref[base + k] = t_ref[k * SR:k * SR + KR, :].astype(bf16)
        wv_ref[base + k] = t_ref[k * SR + KR:(k + 1) * SR, :].astype(bf16)


def build_u(t_ref, u_ref, wu_ref, coords, charge, base):
    half = [0.5 * c for c in coords]
    rows = []
    for h in half:
        a, b, c = split3f(h)
        a, b, c = 2.0 * a, 2.0 * b, 2.0 * c
        rows += [a, a, b, b, a, c]
    one = jnp.ones_like(charge)
    rows += [one, one, one]
    rows += list(split3f(1.0 - half_square(half)))
    put_rows(t_ref, rows, 0)
    put_rows(t_ref, weight_rows(coords, charge), KR)
    for k in range(CLUSTERS):
        u_ref[base + k] = jnp.transpose(t_ref[k * SR:k * SR + KR, :]).astype(bf16)
        wu_ref[base + k] = t_ref[k * SR + KR:(k + 1) * SR, :].astype(bf16)


class Pairs:

    def __init__(self, code_ref, u_ref, v_ref, wu_ref, wv_ref, g_ref, f_ref, rawl_ref, rawr_ref):
        self.code, self.u, self.v, self.wu, self.wv = code_ref, u_ref, v_ref, wu_ref, wv_ref
        self.g, self.f, self.rawl, self.rawr = g_ref, f_ref, rawl_ref, rawr_ref

    def tables(self, place, m):
        q, group = place
        lane = (q & 1) * 64 + group * 8 + m
        ui, vi = self.code[q, 0, lane], self.code[q, 1, lane]
        return jnp.clip(ui, 0, self.u.shape[0] - 1), jnp.clip(vi, 0, self.v.shape[0] - 1)

    def distance(self, place, m, buf):
        ui, vi = self.tables(place, m)
        self.g[buf, m] = jnp.dot(self.u[ui], self.v[vi], preferred_element_type=f32)

    def factor(self, m, buf):
        g0 = self.g[buf, m]
        g = jnp.maximum(g0, 0.0)
        den = 1.125 - g0
        s = pl.reciprocal(den, approx=True)
        t = (g * s) * (2.0 - den * s)
        f = (g * t) * (t + 3.0)
        hi = f.astype(bf16)
        self.f[buf, m, 0] = hi
        self.f[buf, m, 1] = (f - hi.astype(f32)).astype(bf16)

    def sums(self, place, m, buf):
        ui, vi = self.tables(place, m)
        hi, lo = self.f[buf, m, 0], self.f[buf, m, 1]
        both = jnp.concatenate([
            jnp.concatenate([hi, lo], axis=1),
            jnp.concatenate([jnp.transpose(hi), jnp.transpose(lo)], axis=1)], axis=0)
        weights = jnp.concatenate([self.wu[ui], self.wv[vi]], axis=1)
        out = jnp.dot(weights, both, preferred_element_type=f32)
        out = out[:, 0:128] + out[:, 128:256]
        n = place[0] * 64 + place[1] * 8 + m
        self.rawr[pl.ds(n, 8, stride=SLOTS), :] = out[0:8]
        self.rawl[pl.ds(n, 8, stride=SLOTS), :] = out[8:16]

    def stage(self, parity, here, done, factors=True):
        for m in range(NB):
            if done is not None:
                self.sums(done, m, parity)
            if factors:
                self.factor(m, 1 - parity)
            if here is not None:
                self.distance(here, m, parity)


def reduced(raw_ref, hot):
    cols_hi, cols_lo = [], []
    for c in range(4):
        v = raw_ref[c * SLOTS:(c + 1) * SLOTS, :] + raw_ref[(c + 4) * SLOTS:(c + 5) * SLOTS, :]
        hi = v.astype(bf16)
        cols_hi.append(hi)
        cols_lo.append((v - hi.astype(f32)).astype(bf16))
    rhs = jnp.concatenate(
        [jnp.concatenate(cols_hi, axis=1), jnp.concatenate(cols_lo, axis=1)], axis=0)
    return jnp.dot(hot, rhs, preferred_element_type=f32)


def make_hot(code_rows, rows):
    out = []
    for r in code_rows:
        it = lax.broadcasted_iota(i32, (rows, 128), 0)
        out.append(jnp.where(it == r, 1.0, 0.0).astype(bf16))
    one = jnp.concatenate(out, axis=1)
    return jnp.concatenate([one, one], axis=1)


def force_rows(coords, charge, out, row):
    s = out[row:row + 8, 384:512]
    return [charge * (coords[c] * s - out[row:row + 8, c * 128:(c + 1) * 128]) for c in range(3)]


def split3(value):
    hi = value.astype(bf16)
    rest = value - hi.astype(f32)
    mid = rest.astype(bf16)
    lo = (rest - mid.astype(f32)).astype(bf16)
    return hi, mid, lo


def one_hot(atoms_ref):
    slots = atoms_ref.shape[1]
    rows = lax.broadcasted_iota(i32, (ATOMS, slots), 0)
    return jnp.where(rows == atoms_ref[...], 1.0, 0.0).astype(bf16)


def sort_pairs(pairs_ref, code_ref):
    count = pairs_ref.shape[2]
    left, right, t = pairs_ref[0], pairs_ref[1], pairs_ref[2]
    t25 = (t * 5243) >> 17
    t5 = (t * 205) >> 10
    q_row = (t5 - 5 * t25).astype(f32)
    pr_row = (t25 * 5 + t - 5 * t5).astype(f32)
    t_row = t.astype(f32)
    rows = jnp.concatenate([t_row, q_row, pr_row, jnp.zeros((125, count), f32)], axis=0)
    cols = jnp.concatenate(
        [jnp.transpose(rows[:, h * 128:(h + 1) * 128]) for h in range(count // 128)], axis=0)
    t_col, q_col, pr_col = cols[:, 0:1], cols[:, 1:2], cols[:, 2:3]
    a = lax.broadcasted_iota(i32, (count, count), 0)
    b = lax.broadcasted_iota(i32, (count, count), 1)
    same = jnp.where(t_col == t_row, 1.0, 0.0)
    earlier = jnp.where(b < a, 1.0, 0.0)
    rank_row = jnp.sum(same * jnp.where(a < b, 1.0, 0.0), axis=0, keepdims=True)
    rank_col = jnp.sum(same * earlier, axis=1, keepdims=True)
    extra_row = jnp.where(rank_row > 1.5, 1.0, 0.0)
    extra_col = jnp.sum(jnp.where(q_col == q_row, earlier * extra_row, 0.0), axis=1, keepdims=True)
    odd = jnp.where((q_col == 1.0) | (q_col == 3.0), 64.0, 0.0)
    p_col = jnp.floor((pr_col + 0.5) * 0.2)
    r_col = pr_col - 5.0 * p_col
    pi = jnp.where(p_col > 2.0, p_col - 1.0, p_col)
    ri = jnp.where(r_col == 1.0, 0.0, jnp.where(r_col == 3.0, 1.0, jnp.where(r_col == 0.0, 2.0, 3.0)))
    group = jnp.where(p_col == 2.0, 8.0 + 2.0 * ri, 16.0 + 8.0 * ri + 2.0 * pi)
    group = jnp.where(r_col == 2.0, jnp.where(p_col == 2.0, 48.0, 2.0 * pi), group)
    place = jnp.where(rank_col < 1.5, group + rank_col, 50.0 + extra_col)
    place = place + odd + 128.0 * q_col
    lane = lax.broadcasted_iota(i32, (count, 640), 1).astype(f32)
    hot = jnp.where(place == lane, 1.0, 0.0).astype(bf16)
    values = jnp.concatenate(
        [left.astype(f32) + 1.0, right.astype(f32) + 1.0, pr_row, jnp.zeros((13, count), f32)],
        axis=0).astype(bf16)
    out = jnp.dot(values, hot, preferred_element_type=f32)
    for q in range(5):
        code_ref[q] = out[0:8, q * 128:(q + 1) * 128].astype(i32)


def decode(code_in_ref, code_vec_ref, q):
    blk = code_in_ref[q]
    i, j, pr = blk[0:1] - 1, blk[1:2] - 1, blk[2:3]
    code_vec_ref[q, 0:1, :] = q * CLUSTERS + jnp.maximum(i, 0)
    code_vec_ref[q, 1:2, :] = pr * CLUSTERS + jnp.maximum(j, 0)
    code_vec_ref[q, 2:8, :] = jnp.zeros((6, 128), i32)


def sum_rows(code_in_ref):
    left_rows, right_rows = [], []
    high = lax.broadcasted_iota(i32, (1, 128), 1) >= 64
    for h in range(3):
        blk = code_in_ref[2 * h]
        if h < 2:
            blk = blk + code_in_ref[2 * h + 1]
        i, j, pr = blk[0:1] - 1, blk[1:2] - 1, blk[2:3]
        q = 2 * h + (jnp.where(high, 1, 0) if h < 2 else jnp.zeros((1, 128), i32))
        pr = jnp.where(pr < 10, pr, jnp.where(pr < 15, pr + 10, pr - 5))
        left_rows.append(jnp.where(i < 0, -1, q * 8 + i))
        right_rows.append(jnp.where(j < 0, -1, pr * 8 + j))
    return left_rows, right_rows


def kernel(sizes, pairs_hbm, x_hbm, v_hbm, q_hbm, atoms_hbm, x_out, v_out, f_out,
           pairs_ref, x_in, v_in, q_in, atoms_ref,
           plate_ref, tower_ref, vel_ref, fr_ref, fl_ref, landx_ref, landt_ref, landz_ref,
           zsum_ref, code_in_ref, code_send_ref, code_vec_ref, code_ref, slot_ref,
           t_ref, tu_ref, u_ref, v_ref, wu_ref, wv_ref, g_ref, f_ref, rawl_ref, rawr_ref, hr_ref, hl_ref,
           load_sem, local_sem, send_sem, recv_sem):
    me = tuple(lax.axis_index(axis) for axis in AXES)
    column = me[1] & 3
    mirrored = column >= 2
    inner = jnp.where(mirrored, 3 - column, column)

    def tower_at(pos):
        third = jnp.where(inner == 0, 0, 3)
        q = jnp.where(pos == 0, 2, jnp.where(pos == 1, 1, jnp.where(
            pos == 2, third, jnp.where(pos == 3, 3 - third, 4))))
        return jnp.where(mirrored, 4 - q, q)

    def peer(axis, offset):
        n = sizes[axis]
        ids = list(me)
        ids[axis] = lax.rem(me[axis] + (offset + n), n)
        return tuple(ids)

    barrier = pltpu.get_barrier_semaphore()
    partners = [(0, d) for d in (-2, -1, 1, 2)] + [(1, d) for d in (-2, -1, 1, 2)]
    partners += [(2, d) for d in (1, 2, 3)]
    for axis, d in partners:
        pl.semaphore_signal(barrier, 1, device_id=peer(axis, d), device_id_type=MESH)
    loads = [
        pltpu.make_async_copy(src, dst, load_sem.at[n]) for n, (src, dst) in enumerate(
            ((atoms_hbm, atoms_ref), (x_hbm, x_in), (q_hbm, q_in), (v_hbm, v_in), (pairs_hbm, pairs_ref)))]
    for load in loads:
        load.start()

    def copy(step, k, src, dst, to):
        return pltpu.make_async_remote_copy(
            src_ref=src, dst_ref=dst, send_sem=send_sem.at[step, k],
            recv_sem=recv_sem.at[step, k], device_id=to, device_id_type=MESH)

    def comps(step):
        return pl.ds(0, 4) if step == 0 else pl.ds(0, 3)

    def share_z(step, z):
        return copy(step, z, plate_ref.at[step, 2, 0, comps(step)],
                    plate_ref.at[step, 2, z, comps(step)], peer(2, 4 - z))

    def share_t(step, q):
        return copy(step, 4 + q, plate_ref.at[step, 2, 0, comps(step)],
                    tower_ref.at[step, q, comps(step)], peer(1, q - 2))

    def share_p(step, p, z):
        return copy(step, 9 + p * 4 + z, plate_ref.at[step, 2, z, comps(step)],
                    plate_ref.at[step, p, z, comps(step)], peer(0, 2 - p))

    def give_x(step, p, z):
        return copy(step, 29 + p * 4 + z, fr_ref.at[step, p, z], landx_ref.at[step, p, z],
                    peer(0, p - 2))

    def give_t(step, half, q):
        return copy(step, 49 + q, fl_ref.at[step, half, q], landt_ref.at[step, q],
                    peer(1, 2 - q))

    def give_z(step, z):
        return copy(step, 54 + z, zsum_ref.at[step, z], landz_ref.at[step, z], peer(2, z))

    def share_code(q):
        return copy(0, 58 + q, code_send_ref.at[q], code_in_ref.at[q], peer(1, q - 2))

    def to_smem(q):
        return pltpu.make_async_copy(code_vec_ref.at[q], code_ref.at[q], local_sem.at[q])

    with jax.named_scope("slots"):
        plate_ref[0, 2, 0] = jnp.zeros((4, 8, 128), f32)
        vel_ref[...] = jnp.zeros_like(vel_ref)
        rawl_ref[...] = jnp.zeros_like(rawl_ref)
        rawr_ref[...] = jnp.zeros_like(rawr_ref)
        t_ref[...] = jnp.zeros_like(t_ref)
        tu_ref[...] = jnp.zeros_like(tu_ref)
        for load in loads[:4]:
            load.wait()
        data = jnp.concatenate(
            [x_in[c] for c in range(3)] + [q_in[...]] + [v_in[c] for c in range(3)]
            + [jnp.zeros((1, ATOMS), f32)], axis=0)
        hi, mid, lo = split3(data)
        stacked = jnp.concatenate([hi, mid, lo, jnp.zeros_like(hi)], axis=0)
        out = jnp.dot(stacked, one_hot(atoms_ref), preferred_element_type=f32)
        slot = out[0:8] + out[8:16] + out[16:24]
        for k in range(CLUSTERS):
            lanes = slice(k * CLUSTER, (k + 1) * CLUSTER)
            for c in range(4):
                plate_ref[0, 2, 0, c, pl.ds(k, 1), :] = slot[c:c + 1, lanes]
            for c in range(3):
                vel_ref[c, pl.ds(k, 1), :] = slot[4 + c:5 + c, lanes]
    with jax.named_scope("sort"):
        loads[4].wait()
        sort_pairs(pairs_ref, code_send_ref)
        code_in_ref[2] = code_send_ref[2]

    def start_share(step):
        for z in (2, 1, 3):
            share_z(step, z).start()
        for p in SIDE:
            share_p(step, p, 0).start()
        for q in (0, 4, 1, 3):
            share_t(step, q).start()

    with jax.named_scope("barrier"):
        pl.semaphore_wait(barrier, len(partners))
    start_share(0)
    for q in (0, 4, 1, 3):
        share_code(q).start()

    order_of_towers = sum(tower_at(pos) << (3 * pos) for pos in range(5))

    def order(i):
        word = (i * 103) >> 10
        place = 3 * (i - 10 * word)

        def entry(table):
            words = [sum(v << (3 * n) for n, v in enumerate(table[w:w + 10])) for w in range(0, 40, 10)]
            if isinstance(i, int):
                return (words[word] >> place) & 7
            pick = jnp.where(word < 2, jnp.where(word < 1, words[0], words[1]),
                             jnp.where(word < 3, words[2], words[3]))
            return (pick >> place) & 7

        return (order_of_towers >> (3 * entry(POSITIONS))) & 7, entry(GROUPS)

    pairs = Pairs(code_ref, u_ref, v_ref, wu_ref, wv_ref, g_ref, f_ref, rawl_ref, rawr_ref)

    def moved(block, shift):
        return [block[c] if shift[c] is None else block[c] + shift[c] for c in range(3)]

    def plate(step, p, r):
        z = PLACE[r]
        block = [plate_ref[step, p, z, c] for c in range(3)]
        shift = (None if p == 2 else float(p - 2), None, None if r == 2 else float(r - 2))
        return moved(block, shift), plate_ref[0, p, z, 3]

    def tower(step, q):
        if isinstance(q, int) and q == 2:
            return [plate_ref[step, 2, 0, c] for c in range(3)], plate_ref[0, 2, 0, 3]
        shift = (None, jnp.asarray(2 - q, f32), None)
        return moved([tower_ref[step, q, c] for c in range(3)], shift), tower_ref[0, q, 3]

    def v_table(step, p, r):
        coords, charge = plate(step, p, r)
        build_v(t_ref, v_ref, wv_ref, coords, charge, (p * 5 + r) * CLUSTERS)

    def u_table(step, q):
        coords, charge = tower(step, q)
        build_u(tu_ref, u_ref, wu_ref, coords, charge, q * CLUSTERS)

    def tower_in(step, pos):
        q = tower_at(pos)
        share_t(step, q).wait_recv()
        u_table(step, q)

    def codes_in(near):
        for pos in near:
            q = 2 if pos == 0 else tower_at(pos)
            if pos > 0:
                share_code(q).wait_recv()
            decode(code_in_ref, code_vec_ref, q)
            to_smem(q).start()
        for pos in near:
            to_smem(2 if pos == 0 else tower_at(pos)).wait()

    for step in range(STEPS):
        u_table(step, 2)
        v_table(step, 2, 2)
        if step == 0:
            codes_in((0,))
        with jax.named_scope("forward"):
            for z in (1, 3, 2):
                share_z(step, z).wait_recv()
                for p in SIDE:
                    share_p(step, p, z).start()
        with jax.named_scope("near_x"):
            for p in SIDE:
                share_p(step, p, 0).wait_recv()
                v_table(step, p, 2)
        pairs.stage(0, order(0), None, False)
        if step == 0:
            codes_in((1, 2))
        tower_in(step, 1)
        pairs.stage(1, order(1), None)
        tower_in(step, 2)
        pairs.stage(0, order(2), order(0))

        def two_blocks(k, carry):
            i = 3 + 2 * k

            @pl.when(k == 0)
            def _():
                with jax.named_scope("far_x"):
                    for z, r in ((1, 3), (3, 1)):
                        for p in SIDE:
                            share_p(step, p, z).wait_recv()
                            v_table(step, p, r)

            @pl.when(k == 3)
            def _():
                with jax.named_scope("far_x2"):
                    for p in SIDE:
                        share_p(step, p, 2).wait_recv()
                        v_table(step, p, 0)
                        v_table(step, p, 4)
                    for r in SIDE:
                        v_table(step, 2, r)

            @pl.when(k == 6)
            def _():
                with jax.named_scope("tower3"):
                    if step == 0:
                        codes_in((3, 4))
                    tower_in(step, 3)

            @pl.when(k == 8)
            def _():
                with jax.named_scope("tower4"):
                    tower_in(step, 4)

            here, later = order(i), order(i + 1)
            pairs.stage(1, here, carry[0:2])
            pairs.stage(0, later, carry[2:4])
            return here + later

        with jax.named_scope("loop"):
            last = lax.fori_loop(0, 15, two_blocks, tuple(
                jnp.asarray(v, i32) for v in order(1) + order(2)))
        pairs.stage(1, order(33), last[0:2])
        with jax.named_scope("first_sums"):
            if step == 0:
                left_rows, right_rows = sum_rows(code_in_ref)
                hl_ref[...] = make_hot(left_rows, 40)
                hr_ref[...] = make_hot(right_rows, 200)
            out = reduced(rawr_ref, hr_ref[0:160])
            for z, rs in ((2, (0, 4)), (1, (3,)), (3, (1,)), (0, (2,))):
                for n, p in enumerate(SIDE):
                    parts = [force_rows(*plate(step, p, r), out, (n * 5 + r) * 8) for r in rs]
                    for c in range(3):
                        fr_ref[step, p, z, c] = sum(part[c] for part in parts[1:]) + parts[0][c] if (
                            len(parts) > 1) else parts[0][c]
                    give_x(step, p, z).start()
            out = reduced(rawl_ref, hl_ref[...])
            for q in SIDE:
                part = force_rows(*tower(step, q), out, q * 8)
                for c in range(3):
                    fl_ref[step, 0, q, c] = part[c]
            for pos in (4, 3):
                give_t(step, 0, tower_at(pos)).start()
        with jax.named_scope("late"):
            pairs.stage(0, order(34), last[2:4])
            pairs.stage(1, None, order(33))
            pairs.stage(0, None, order(34), False)
        with jax.named_scope("last_sums"):
            out = reduced(rawl_ref, hl_ref[...])
            for q in range(5):
                part = force_rows(*tower(step, q), out, q * 8)
                for c in range(3):
                    fl_ref[step, 1, q, c] = part[c]
            for pos in (2, 1):
                give_t(step, 1, tower_at(pos)).start()
            out = reduced(rawr_ref, hr_ref[160:200])
            parts = [force_rows(*plate(step, 2, r), out, r * 8) for r in range(5)]
        total = {2: [a + b for a, b in zip(parts[0], parts[4])], 1: parts[3], 3: parts[1], 0: parts[2]}
        for z in (2, 1, 3, 0):
            with jax.named_scope("give_x"):
                for p in SIDE:
                    give_x(step, p, z).wait_recv()
            for p in SIDE:
                total[z] = [total[z][c] + landx_ref[step, p, z, c] for c in range(3)]
            if z > 0:
                for c in range(3):
                    zsum_ref[step, z, c] = total[z][c]
                give_z(step, z).start()
        force = [total[0][c] + fl_ref[step, 1, 2, c] for c in range(3)]
        with jax.named_scope("give_t"):
            for q in SIDE:
                give_t(step, 0, q).wait_recv()
        for q in SIDE:
            force = [force[c] + landt_ref[step, q, c] for c in range(3)]
        with jax.named_scope("give_z"):
            for z in (1, 3, 2):
                give_z(step, z).wait_recv()
        for z in (1, 3, 2):
            force = [force[c] + landz_ref[step, z, c] for c in range(3)]
        velocity = [vel_ref[c] + TIME_STEP * force[c] for c in range(3)]
        coords = [plate_ref[step, 2, 0, c] + TIME_STEP * velocity[c] for c in range(3)]
        if step < STEPS - 1:
            for c in range(3):
                plate_ref[step + 1, 2, 0, c] = coords[c]
            start_share(step + 1)
            for c in range(3):
                vel_ref[c] = velocity[c]

    with jax.named_scope("output"):
        slot_ref[...] = jnp.zeros_like(slot_ref)
        for k in range(CLUSTERS):
            lanes = slice(k * CLUSTER, (k + 1) * CLUSTER)
            for c in range(3):
                slot_ref[pl.ds(c, 1), lanes] = coords[c][k:k + 1]
                slot_ref[pl.ds(3 + c, 1), lanes] = velocity[c][k:k + 1]
                slot_ref[pl.ds(6 + c, 1), lanes] = force[c][k:k + 1]
        stacked = jnp.concatenate(split3(slot_ref[...]), axis=0)
        out = lax.dot_general(
            stacked, one_hot(atoms_ref), (((1,), (1,)), ((), ())), preferred_element_type=f32)
        atom = out[0:16] + out[16:32] + out[32:48]
        for c in range(3):
            x_out[c] = atom[c:c + 1]
            v_out[c] = atom[3 + c:4 + c]
            f_out[c] = atom[6 + c:7 + c]

    for step in range(STEPS):
        for z in (1, 2, 3):
            share_z(step, z).wait_send()
            give_z(step, z).wait_send()
        for s in SIDE:
            share_t(step, s).wait_send()
            for z in range(4):
                share_p(step, s, z).wait_send()
                give_x(step, s, z).wait_send()
        for pos in (4, 3):
            give_t(step, 0, tower_at(pos)).wait_send()
        for pos in (2, 1):
            give_t(step, 1, tower_at(pos)).wait_send()
    for q in SIDE:
        share_code(q).wait_send()


def shards(sizes, positions, velocities, charges, cluster_atoms, pair_list):
    slots = cluster_atoms.shape[-1]
    x = positions.reshape(3, 1, ATOMS)
    v = velocities.reshape(3, 1, ATOMS)
    q = charges.reshape(1, ATOMS)
    atoms = cluster_atoms.reshape(1, slots)
    pairs = pair_list.reshape(3, 1, pair_list.shape[-1])
    shape = jax.ShapeDtypeStruct((3, 1, ATOMS), f32)
    vmem = pl.BlockSpec(memory_space=pltpu.VMEM)
    outs = pl.pallas_call(
        functools.partial(kernel, sizes),
        out_shape=(shape, shape, shape),
        in_specs=[pl.BlockSpec(memory_space=pl.ANY)] * 5,
        out_specs=(vmem, vmem, vmem),
        scratch_shapes=[
            pltpu.VMEM(pairs.shape, i32),
            pltpu.VMEM(x.shape, f32),
            pltpu.VMEM(v.shape, f32),
            pltpu.VMEM(q.shape, f32),
            pltpu.VMEM(atoms.shape, i32),
            pltpu.VMEM((STEPS, 5, 4, 4, 8, 128), f32),
            pltpu.VMEM((STEPS, 5, 4, 8, 128), f32),
            pltpu.VMEM((3, 8, 128), f32),
            pltpu.VMEM((STEPS, 5, 4, 3, 8, 128), f32),
            pltpu.VMEM((STEPS, 2, 5, 3, 8, 128), f32),
            pltpu.VMEM((STEPS, 5, 4, 3, 8, 128), f32),
            pltpu.VMEM((STEPS, 5, 3, 8, 128), f32),
            pltpu.VMEM((STEPS, 4, 3, 8, 128), f32),
            pltpu.VMEM((STEPS, 4, 3, 8, 128), f32),
            pltpu.VMEM((5, 8, 128), i32),
            pltpu.VMEM((5, 8, 128), i32),
            pltpu.VMEM((5, 8, 128), i32),
            pltpu.SMEM((5, 8, 128), i32),
            pltpu.VMEM((16, slots), f32),
            pltpu.VMEM((9 * SR, 128), f32),
            pltpu.VMEM((9 * SR, 128), f32),
            pltpu.VMEM((30, 128, KR), bf16),
            pltpu.VMEM((150, KR, 128), bf16),
            pltpu.VMEM((30, 16, 128), bf16),
            pltpu.VMEM((150, 16, 128), bf16),
            pltpu.VMEM((2, NB, 128, 128), f32),
            pltpu.VMEM((2, NB, 2, 128, 128), bf16),
            pltpu.VMEM((9 * SLOTS, 128), f32),
            pltpu.VMEM((9 * SLOTS, 128), f32),
            pltpu.VMEM((200, 2 * SLOTS), bf16),
            pltpu.VMEM((40, 2 * SLOTS), bf16),
            pltpu.SemaphoreType.DMA((5,)),
            pltpu.SemaphoreType.DMA((5,)),
            pltpu.SemaphoreType.DMA((STEPS, 63)),
            pltpu.SemaphoreType.DMA((STEPS, 63)),
        ],
        compiler_params=pltpu.CompilerParams(collective_id=0, has_side_effects=True),
        name="leapfrog",
    )(pairs, x, v, q, atoms)
    return tuple(out.reshape(positions.shape) for out in outs)


def solution(mesh):
    spec3 = P(None, "gx", "gy", "gz", None)
    spec1 = P("gx", "gy", "gz", None)
    sizes = tuple(mesh.shape[axis] for axis in AXES)
    return jax.shard_map(
        functools.partial(shards, sizes),
        mesh=mesh,
        in_specs=(spec3, spec3, spec1, spec1, spec3),
        out_specs=(spec3, spec3, spec3),
        check_vma=False,
    )
```

```python
import functools

import jax
import jax.numpy as jnp
from jax import lax
from jax.experimental import pallas as pl
from jax.experimental.pallas import tpu as pltpu
from jax.sharding import PartitionSpec as P

f32, bf16, i32 = jnp.float32, jnp.bfloat16, jnp.int32
MESH = pl.DeviceIdType.MESH
AXES = ("gx", "gy", "gz")
CLUSTER = 128
CLUSTERS = 6
ATOMS = 512
STEPS = 2
TIME_STEP = 0.02
NB = 8
KR = 32
SR = 48
SLOTS = 384
PLACE = (2, 3, 0, 1, 2)
SIDE = (0, 1, 3, 4)
POSITIONS = (0, 1, 2, 0, 1, 2, 0, 1, 2, 0, 1, 2, 0, 1, 2, 3, 3, 3, 3, 3, 4, 4, 4, 4, 4, 0, 1, 2, 3, 4, 3, 4, 0, 1, 2)
GROUPS = (0, 0, 0, 2, 2, 2, 3, 3, 3, 4, 4, 4, 5, 5, 5, 0, 2, 3, 4, 5, 0, 2, 3, 4, 5, 6, 6, 6, 6, 6, 1, 1, 1, 1, 1)


def split2(v):
    hi = v.astype(bf16).astype(f32)
    return hi, v - hi


def split3f(v):
    a = v.astype(bf16).astype(f32)
    r = v - a
    b = r.astype(bf16).astype(f32)
    return a, b, r - b


def weight_rows(coords, charge):
    q = 0.125 * charge
    parts = [split2(q * c) for c in coords] + [split2(q)]
    return [a for a, _ in parts] + [b for _, b in parts]


def put_rows(t_ref, rows, base):
    for n, r in enumerate(rows):
        t_ref[pl.ds(base + n, 8, stride=SR), :] = r


def half_square(half):
    return half[0] * half[0] + half[1] * half[1] + half[2] * half[2]


def build_v(t_ref, v_ref, wv_ref, coords, charge, base):
    half = [0.5 * c for c in coords]
    rows = []
    for h in half:
        a, b, c = split3f(h)
        rows += [a, b, a, b, c, a]
    rows += list(split3f(-half_square(half)))
    one = jnp.ones_like(charge)
    rows += [one, one, one]
    put_rows(t_ref, rows, 0)
    put_rows(t_ref, weight_rows(coords, charge), KR + 8)
    for k in range(CLUSTERS):
        v_ref[base + k] = t_ref[k * SR:k * SR + KR, :].astype(bf16)
        wv_ref[base + k] = t_ref[k * SR + KR:(k + 1) * SR, :].astype(bf16)


def build_u(t_ref, u_ref, wu_ref, coords, charge, base):
    half = [0.5 * c for c in coords]
    rows = []
    for h in half:
        a, b, c = split3f(h)
        a, b, c = 2.0 * a, 2.0 * b, 2.0 * c
        rows += [a, a, b, b, a, c]
    one = jnp.ones_like(charge)
    rows += [one, one, one]
    rows += list(split3f(1.0 - half_square(half)))
    put_rows(t_ref, rows, 0)
    put_rows(t_ref, weight_rows(coords, charge), KR)
    for k in range(CLUSTERS):
        u_ref[base + k] = jnp.transpose(t_ref[k * SR:k * SR + KR, :]).astype(bf16)
        wu_ref[base + k] = t_ref[k * SR + KR:(k + 1) * SR, :].astype(bf16)


class Pairs:

    def __init__(self, code_ref, u_ref, v_ref, wu_ref, wv_ref, g_ref, f_ref, rawl_ref, rawr_ref):
        self.code, self.u, self.v, self.wu, self.wv = code_ref, u_ref, v_ref, wu_ref, wv_ref
        self.g, self.f, self.rawl, self.rawr = g_ref, f_ref, rawl_ref, rawr_ref

    def tables(self, place, m):
        q, group = place
        lane = (q & 1) * 64 + group * 8 + m
        ui, vi = self.code[q, 0, lane], self.code[q, 1, lane]
        return jnp.clip(ui, 0, self.u.shape[0] - 1), jnp.clip(vi, 0, self.v.shape[0] - 1)

    def distance(self, place, m, buf):
        ui, vi = self.tables(place, m)
        self.g[buf, m] = jnp.dot(self.u[ui], self.v[vi], preferred_element_type=f32)

    def factor(self, m, buf):
        g0 = self.g[buf, m]
        g = jnp.maximum(g0, 0.0)
        den = 1.125 - g0
        s = pl.reciprocal(den, approx=True)
        t = (g * s) * (2.0 - den * s)
        f = (g * t) * (t + 3.0)
        hi = f.astype(bf16)
        self.f[buf, m, 0] = hi
        self.f[buf, m, 1] = (f - hi.astype(f32)).astype(bf16)

    def sums(self, place, m, buf):
        ui, vi = self.tables(place, m)
        hi, lo = self.f[buf, m, 0], self.f[buf, m, 1]
        both = jnp.concatenate([
            jnp.concatenate([hi, lo], axis=1),
            jnp.concatenate([jnp.transpose(hi), jnp.transpose(lo)], axis=1)], axis=0)
        weights = jnp.concatenate([self.wu[ui], self.wv[vi]], axis=1)
        out = jnp.dot(weights, both, preferred_element_type=f32)
        out = out[:, 0:128] + out[:, 128:256]
        n = pl.multiple_of(8 * (place[0] * 64 + place[1] * 8 + m), 8)
        self.rawr[pl.ds(n, 8), :] = out[0:8]
        self.rawl[pl.ds(n, 8), :] = out[8:16]

    def stage(self, parity, here, done, factors=True):
        for m in range(NB):
            if done is not None:
                self.sums(done, m, parity)
            if factors:
                self.factor(m, 1 - parity)
            if here is not None:
                self.distance(here, m, parity)


def reduced(raw_ref, hot):
    cols_hi, cols_lo = [], []
    for c in range(4):
        v = raw_ref[pl.ds(c, SLOTS, stride=8), :] + raw_ref[pl.ds(c + 4, SLOTS, stride=8), :]
        hi = v.astype(bf16)
        cols_hi.append(hi)
        cols_lo.append((v - hi.astype(f32)).astype(bf16))
    rhs = jnp.concatenate(
        [jnp.concatenate(cols_hi, axis=1), jnp.concatenate(cols_lo, axis=1)], axis=0)
    return jnp.dot(hot, rhs, preferred_element_type=f32)


def make_hot(code_rows, rows):
    out = []
    for r in code_rows:
        it = lax.broadcasted_iota(i32, (rows, 128), 0)
        out.append(jnp.where(it == r, 1.0, 0.0).astype(bf16))
    one = jnp.concatenate(out, axis=1)
    return jnp.concatenate([one, one], axis=1)


def force_rows(coords, charge, out, row):
    s = out[row:row + 8, 384:512]
    return [charge * (coords[c] * s - out[row:row + 8, c * 128:(c + 1) * 128]) for c in range(3)]


def split3(value):
    hi = value.astype(bf16)
    rest = value - hi.astype(f32)
    mid = rest.astype(bf16)
    lo = (rest - mid.astype(f32)).astype(bf16)
    return hi, mid, lo


def one_hot(atoms_ref):
    slots = atoms_ref.shape[1]
    rows = lax.broadcasted_iota(i32, (ATOMS, slots), 0)
    return jnp.where(rows == atoms_ref[...], 1.0, 0.0).astype(bf16)


def sort_pairs(pairs_ref, code_ref):
    count = pairs_ref.shape[2]
    left, right, t = pairs_ref[0], pairs_ref[1], pairs_ref[2]
    t25 = (t * 5243) >> 17
    t5 = (t * 205) >> 10
    q_row = (t5 - 5 * t25).astype(f32)
    pr_row = (t25 * 5 + t - 5 * t5).astype(f32)
    t_row = t.astype(f32)
    rows = jnp.concatenate([t_row, q_row, pr_row, jnp.zeros((125, count), f32)], axis=0)
    cols = jnp.concatenate(
        [jnp.transpose(rows[:, h * 128:(h + 1) * 128]) for h in range(count // 128)], axis=0)
    t_col, q_col, pr_col = cols[:, 0:1], cols[:, 1:2], cols[:, 2:3]
    a = lax.broadcasted_iota(i32, (count, count), 0)
    b = lax.broadcasted_iota(i32, (count, count), 1)
    same = jnp.where(t_col == t_row, 1.0, 0.0)
    earlier = jnp.where(b < a, 1.0, 0.0)
    rank_row = jnp.sum(same * jnp.where(a < b, 1.0, 0.0), axis=0, keepdims=True)
    rank_col = jnp.sum(same * earlier, axis=1, keepdims=True)
    extra_row = jnp.where(rank_row > 1.5, 1.0, 0.0)
    extra_col = jnp.sum(jnp.where(q_col == q_row, earlier * extra_row, 0.0), axis=1, keepdims=True)
    odd = jnp.where((q_col == 1.0) | (q_col == 3.0), 64.0, 0.0)
    p_col = jnp.floor((pr_col + 0.5) * 0.2)
    r_col = pr_col - 5.0 * p_col
    pi = jnp.where(p_col > 2.0, p_col - 1.0, p_col)
    ri = jnp.where(r_col == 1.0, 0.0, jnp.where(r_col == 3.0, 1.0, jnp.where(r_col == 0.0, 2.0, 3.0)))
    group = jnp.where(p_col == 2.0, 8.0 + 2.0 * ri, 16.0 + 8.0 * ri + 2.0 * pi)
    group = jnp.where(r_col == 2.0, jnp.where(p_col == 2.0, 48.0, 2.0 * pi), group)
    place = jnp.where(rank_col < 1.5, group + rank_col, 50.0 + extra_col)
    place = place + odd + 128.0 * q_col
    lane = lax.broadcasted_iota(i32, (count, 640), 1).astype(f32)
    hot = jnp.where(place == lane, 1.0, 0.0).astype(bf16)
    values = jnp.concatenate(
        [left.astype(f32) + 1.0, right.astype(f32) + 1.0, pr_row, jnp.zeros((13, count), f32)],
        axis=0).astype(bf16)
    out = jnp.dot(values, hot, preferred_element_type=f32)
    for q in range(5):
        code_ref[q] = out[0:8, q * 128:(q + 1) * 128].astype(i32)


def decode(code_in_ref, code_vec_ref, q):
    blk = code_in_ref[q]
    i, j, pr = blk[0:1] - 1, blk[1:2] - 1, blk[2:3]
    code_vec_ref[q, 0:1, :] = q * CLUSTERS + jnp.maximum(i, 0)
    code_vec_ref[q, 1:2, :] = pr * CLUSTERS + jnp.maximum(j, 0)
    code_vec_ref[q, 2:8, :] = jnp.zeros((6, 128), i32)


def sum_rows(code_in_ref):
    left_rows, right_rows = [], []
    high = lax.broadcasted_iota(i32, (1, 128), 1) >= 64
    for h in range(3):
        blk = code_in_ref[2 * h]
        if h < 2:
            blk = blk + code_in_ref[2 * h + 1]
        i, j, pr = blk[0:1] - 1, blk[1:2] - 1, blk[2:3]
        q = 2 * h + (jnp.where(high, 1, 0) if h < 2 else jnp.zeros((1, 128), i32))
        pr = jnp.where(pr < 10, pr, jnp.where(pr < 15, pr + 10, pr - 5))
        left_rows.append(jnp.where(i < 0, -1, q * 8 + i))
        right_rows.append(jnp.where(j < 0, -1, pr * 8 + j))
    return left_rows, right_rows


def kernel(sizes, pairs_hbm, x_hbm, v_hbm, q_hbm, atoms_hbm, x_out, v_out, f_out,
           pairs_ref, x_in, v_in, q_in, atoms_ref,
           plate_ref, tower_ref, vel_ref, fr_ref, fl_ref, landx_ref, landt_ref, landz_ref,
           zsum_ref, code_in_ref, code_send_ref, code_vec_ref, code_ref, slot_ref,
           t_ref, tu_ref, u_ref, v_ref, wu_ref, wv_ref, g_ref, f_ref, rawl_ref, rawr_ref, hr_ref, hl_ref,
           load_sem, local_sem, send_sem, recv_sem):
    me = tuple(lax.axis_index(axis) for axis in AXES)
    column = me[1] & 3
    mirrored = column >= 2
    inner = jnp.where(mirrored, 3 - column, column)

    def tower_at(pos):
        third = jnp.where(inner == 0, 0, 3)
        q = jnp.where(pos == 0, 2, jnp.where(pos == 1, 1, jnp.where(
            pos == 2, third, jnp.where(pos == 3, 3 - third, 4))))
        return jnp.where(mirrored, 4 - q, q)

    def peer(axis, offset):
        n = sizes[axis]
        ids = list(me)
        ids[axis] = lax.rem(me[axis] + (offset + n), n)
        return tuple(ids)

    barrier = pltpu.get_barrier_semaphore()
    partners = [(0, d) for d in (-2, -1, 1, 2)] + [(1, d) for d in (-2, -1, 1, 2)]
    partners += [(2, d) for d in (1, 2, 3)]
    for axis, d in partners:
        pl.semaphore_signal(barrier, 1, device_id=peer(axis, d), device_id_type=MESH)
    loads = [
        pltpu.make_async_copy(src, dst, load_sem.at[n]) for n, (src, dst) in enumerate(
            ((atoms_hbm, atoms_ref), (x_hbm, x_in), (q_hbm, q_in), (v_hbm, v_in), (pairs_hbm, pairs_ref)))]
    for load in loads:
        load.start()

    def copy(step, k, src, dst, to):
        return pltpu.make_async_remote_copy(
            src_ref=src, dst_ref=dst, send_sem=send_sem.at[step, k],
            recv_sem=recv_sem.at[step, k], device_id=to, device_id_type=MESH)

    def comps(step):
        return pl.ds(0, 4) if step == 0 else pl.ds(0, 3)

    def share_z(step, z):
        return copy(step, z, plate_ref.at[step, 2, 0, comps(step)],
                    plate_ref.at[step, 2, z, comps(step)], peer(2, 4 - z))

    def share_t(step, q):
        return copy(step, 4 + q, plate_ref.at[step, 2, 0, comps(step)],
                    tower_ref.at[step, q, comps(step)], peer(1, q - 2))

    def share_p(step, p, z):
        return copy(step, 9 + p * 4 + z, plate_ref.at[step, 2, z, comps(step)],
                    plate_ref.at[step, p, z, comps(step)], peer(0, 2 - p))

    def give_x(step, p, z):
        return copy(step, 29 + p * 4 + z, fr_ref.at[step, p, z], landx_ref.at[step, p, z],
                    peer(0, p - 2))

    def give_t(step, half, q):
        return copy(step, 49 + q, fl_ref.at[step, half, q], landt_ref.at[step, q],
                    peer(1, 2 - q))

    def give_z(step, z):
        return copy(step, 54 + z, zsum_ref.at[step, z], landz_ref.at[step, z], peer(2, z))

    def share_code(q):
        return copy(0, 58 + q, code_send_ref.at[q], code_in_ref.at[q], peer(1, q - 2))

    def to_smem(q):
        return pltpu.make_async_copy(code_vec_ref.at[q], code_ref.at[q], local_sem.at[q])

    with jax.named_scope("slots"):
        plate_ref[0, 2, 0] = jnp.zeros((4, 8, 128), f32)
        vel_ref[...] = jnp.zeros_like(vel_ref)
        rawl_ref[...] = jnp.zeros_like(rawl_ref)
        rawr_ref[...] = jnp.zeros_like(rawr_ref)
        t_ref[...] = jnp.zeros_like(t_ref)
        tu_ref[...] = jnp.zeros_like(tu_ref)
        for load in loads[:4]:
            load.wait()
        data = jnp.concatenate(
            [x_in[c] for c in range(3)] + [q_in[...]] + [v_in[c] for c in range(3)]
            + [jnp.zeros((1, ATOMS), f32)], axis=0)
        hi, mid, lo = split3(data)
        stacked = jnp.concatenate([hi, mid, lo, jnp.zeros_like(hi)], axis=0)
        out = jnp.dot(stacked, one_hot(atoms_ref), preferred_element_type=f32)
        slot = out[0:8] + out[8:16] + out[16:24]
        for k in range(CLUSTERS):
            lanes = slice(k * CLUSTER, (k + 1) * CLUSTER)
            for c in range(4):
                plate_ref[0, 2, 0, c, pl.ds(k, 1), :] = slot[c:c + 1, lanes]
            for c in range(3):
                vel_ref[c, pl.ds(k, 1), :] = slot[4 + c:5 + c, lanes]
    with jax.named_scope("sort"):
        loads[4].wait()
        sort_pairs(pairs_ref, code_send_ref)
        code_in_ref[2] = code_send_ref[2]

    def start_share(step):
        for z in (2, 1, 3):
            share_z(step, z).start()
        for p in SIDE:
            share_p(step, p, 0).start()
        for q in (0, 4, 1, 3):
            share_t(step, q).start()

    with jax.named_scope("barrier"):
        pl.semaphore_wait(barrier, len(partners))
    start_share(0)
    for q in (0, 4, 1, 3):
        share_code(q).start()

    order_of_towers = sum(tower_at(pos) << (3 * pos) for pos in range(5))

    def order(i):
        word = (i * 103) >> 10
        place = 3 * (i - 10 * word)

        def entry(table):
            words = [sum(v << (3 * n) for n, v in enumerate(table[w:w + 10])) for w in range(0, 40, 10)]
            if isinstance(i, int):
                return (words[word] >> place) & 7
            pick = jnp.where(word < 2, jnp.where(word < 1, words[0], words[1]),
                             jnp.where(word < 3, words[2], words[3]))
            return (pick >> place) & 7

        return (order_of_towers >> (3 * entry(POSITIONS))) & 7, entry(GROUPS)

    pairs = Pairs(code_ref, u_ref, v_ref, wu_ref, wv_ref, g_ref, f_ref, rawl_ref, rawr_ref)

    def moved(block, shift):
        return [block[c] if shift[c] is None else block[c] + shift[c] for c in range(3)]

    def plate(step, p, r):
        z = PLACE[r]
        block = [plate_ref[step, p, z, c] for c in range(3)]
        shift = (None if p == 2 else float(p - 2), None, None if r == 2 else float(r - 2))
        return moved(block, shift), plate_ref[0, p, z, 3]

    def tower(step, q):
        if isinstance(q, int) and q == 2:
            return [plate_ref[step, 2, 0, c] for c in range(3)], plate_ref[0, 2, 0, 3]
        shift = (None, jnp.asarray(2 - q, f32), None)
        return moved([tower_ref[step, q, c] for c in range(3)], shift), tower_ref[0, q, 3]

    def v_table(step, p, r):
        coords, charge = plate(step, p, r)
        build_v(t_ref, v_ref, wv_ref, coords, charge, (p * 5 + r) * CLUSTERS)

    def u_table(step, q):
        coords, charge = tower(step, q)
        build_u(tu_ref, u_ref, wu_ref, coords, charge, q * CLUSTERS)

    def tower_in(step, pos):
        q = tower_at(pos)
        share_t(step, q).wait_recv()
        u_table(step, q)

    def codes_in(near):
        for pos in near:
            q = 2 if pos == 0 else tower_at(pos)
            if pos > 0:
                share_code(q).wait_recv()
            decode(code_in_ref, code_vec_ref, q)
            to_smem(q).start()
        for pos in near:
            to_smem(2 if pos == 0 else tower_at(pos)).wait()

    for step in range(STEPS):
        u_table(step, 2)
        v_table(step, 2, 2)
        if step == 0:
            codes_in((0,))
        with jax.named_scope("forward"):
            for z in (1, 3, 2):
                share_z(step, z).wait_recv()
                for p in SIDE:
                    share_p(step, p, z).start()
        with jax.named_scope("near_x"):
            for p in SIDE:
                share_p(step, p, 0).wait_recv()
                v_table(step, p, 2)
        pairs.stage(0, order(0), None, False)
        if step == 0:
            codes_in((1, 2))
        tower_in(step, 1)
        pairs.stage(1, order(1), None)
        tower_in(step, 2)
        pairs.stage(0, order(2), order(0))

        def two_blocks(k, carry):
            i = 3 + 2 * k

            @pl.when(k == 0)
            def _():
                with jax.named_scope("far_x"):
                    for z, r in ((1, 3), (3, 1)):
                        for p in SIDE:
                            share_p(step, p, z).wait_recv()
                            v_table(step, p, r)

            @pl.when(k == 3)
            def _():
                with jax.named_scope("far_x2"):
                    for p in SIDE:
                        share_p(step, p, 2).wait_recv()
                        v_table(step, p, 0)
                        v_table(step, p, 4)
                    for r in SIDE:
                        v_table(step, 2, r)

            @pl.when(k == 6)
            def _():
                with jax.named_scope("tower3"):
                    if step == 0:
                        codes_in((3, 4))
                    tower_in(step, 3)

            @pl.when(k == 8)
            def _():
                with jax.named_scope("tower4"):
                    tower_in(step, 4)

            here, later = order(i), order(i + 1)
            pairs.stage(1, here, carry[0:2])
            pairs.stage(0, later, carry[2:4])
            return here + later

        with jax.named_scope("loop"):
            last = lax.fori_loop(0, 15, two_blocks, tuple(
                jnp.asarray(v, i32) for v in order(1) + order(2)))
        pairs.stage(1, order(33), last[0:2])
        with jax.named_scope("first_sums"):
            if step == 0:
                left_rows, right_rows = sum_rows(code_in_ref)
                hl_ref[...] = make_hot(left_rows, 40)
                hr_ref[...] = make_hot(right_rows, 200)
            out = reduced(rawr_ref, hr_ref[0:160])
            for z, rs in ((2, (0, 4)), (1, (3,)), (3, (1,)), (0, (2,))):
                for n, p in enumerate(SIDE):
                    parts = [force_rows(*plate(step, p, r), out, (n * 5 + r) * 8) for r in rs]
                    for c in range(3):
                        fr_ref[step, p, z, c] = sum(part[c] for part in parts[1:]) + parts[0][c] if (
                            len(parts) > 1) else parts[0][c]
                    give_x(step, p, z).start()
            out = reduced(rawl_ref, hl_ref[...])
            for q in SIDE:
                part = force_rows(*tower(step, q), out, q * 8)
                for c in range(3):
                    fl_ref[step, 0, q, c] = part[c]
            for pos in (4, 3):
                give_t(step, 0, tower_at(pos)).start()
        with jax.named_scope("late"):
            pairs.stage(0, order(34), last[2:4])
            pairs.stage(1, None, order(33))
            pairs.stage(0, None, order(34), False)
        with jax.named_scope("last_sums"):
            out = reduced(rawl_ref, hl_ref[...])
            for q in range(5):
                part = force_rows(*tower(step, q), out, q * 8)
                for c in range(3):
                    fl_ref[step, 1, q, c] = part[c]
            for pos in (2, 1):
                give_t(step, 1, tower_at(pos)).start()
            out = reduced(rawr_ref, hr_ref[160:200])
            parts = [force_rows(*plate(step, 2, r), out, r * 8) for r in range(5)]
        total = {2: [a + b for a, b in zip(parts[0], parts[4])], 1: parts[3], 3: parts[1], 0: parts[2]}
        for z in (2, 1, 3, 0):
            with jax.named_scope("give_x"):
                for p in SIDE:
                    give_x(step, p, z).wait_recv()
            for p in SIDE:
                total[z] = [total[z][c] + landx_ref[step, p, z, c] for c in range(3)]
            if z > 0:
                for c in range(3):
                    zsum_ref[step, z, c] = total[z][c]
                give_z(step, z).start()
        force = [total[0][c] + fl_ref[step, 1, 2, c] for c in range(3)]
        with jax.named_scope("give_t"):
            for q in SIDE:
                give_t(step, 0, q).wait_recv()
        for q in SIDE:
            force = [force[c] + landt_ref[step, q, c] for c in range(3)]
        with jax.named_scope("give_z"):
            for z in (1, 3, 2):
                give_z(step, z).wait_recv()
        for z in (1, 3, 2):
            force = [force[c] + landz_ref[step, z, c] for c in range(3)]
        velocity = [vel_ref[c] + TIME_STEP * force[c] for c in range(3)]
        coords = [plate_ref[step, 2, 0, c] + TIME_STEP * velocity[c] for c in range(3)]
        if step < STEPS - 1:
            for c in range(3):
                plate_ref[step + 1, 2, 0, c] = coords[c]
            start_share(step + 1)
            for c in range(3):
                vel_ref[c] = velocity[c]

    with jax.named_scope("output"):
        slot_ref[...] = jnp.zeros_like(slot_ref)
        for k in range(CLUSTERS):
            lanes = slice(k * CLUSTER, (k + 1) * CLUSTER)
            for c in range(3):
                slot_ref[pl.ds(c, 1), lanes] = coords[c][k:k + 1]
                slot_ref[pl.ds(3 + c, 1), lanes] = velocity[c][k:k + 1]
                slot_ref[pl.ds(6 + c, 1), lanes] = force[c][k:k + 1]
        stacked = jnp.concatenate(split3(slot_ref[...]), axis=0)
        out = lax.dot_general(
            stacked, one_hot(atoms_ref), (((1,), (1,)), ((), ())), preferred_element_type=f32)
        atom = out[0:16] + out[16:32] + out[32:48]
        for c in range(3):
            x_out[c] = atom[c:c + 1]
            v_out[c] = atom[3 + c:4 + c]
            f_out[c] = atom[6 + c:7 + c]

    for step in range(STEPS):
        for z in (1, 2, 3):
            share_z(step, z).wait_send()
            give_z(step, z).wait_send()
        for s in SIDE:
            share_t(step, s).wait_send()
            for z in range(4):
                share_p(step, s, z).wait_send()
                give_x(step, s, z).wait_send()
        for pos in (4, 3):
            give_t(step, 0, tower_at(pos)).wait_send()
        for pos in (2, 1):
            give_t(step, 1, tower_at(pos)).wait_send()
    for q in SIDE:
        share_code(q).wait_send()


def shards(sizes, positions, velocities, charges, cluster_atoms, pair_list):
    slots = cluster_atoms.shape[-1]
    x = positions.reshape(3, 1, ATOMS)
    v = velocities.reshape(3, 1, ATOMS)
    q = charges.reshape(1, ATOMS)
    atoms = cluster_atoms.reshape(1, slots)
    pairs = pair_list.reshape(3, 1, pair_list.shape[-1])
    shape = jax.ShapeDtypeStruct((3, 1, ATOMS), f32)
    vmem = pl.BlockSpec(memory_space=pltpu.VMEM)
    outs = pl.pallas_call(
        functools.partial(kernel, sizes),
        out_shape=(shape, shape, shape),
        in_specs=[pl.BlockSpec(memory_space=pl.ANY)] * 5,
        out_specs=(vmem, vmem, vmem),
        scratch_shapes=[
            pltpu.VMEM(pairs.shape, i32),
            pltpu.VMEM(x.shape, f32),
            pltpu.VMEM(v.shape, f32),
            pltpu.VMEM(q.shape, f32),
            pltpu.VMEM(atoms.shape, i32),
            pltpu.VMEM((STEPS, 5, 4, 4, 8, 128), f32),
            pltpu.VMEM((STEPS, 5, 4, 8, 128), f32),
            pltpu.VMEM((3, 8, 128), f32),
            pltpu.VMEM((STEPS, 5, 4, 3, 8, 128), f32),
            pltpu.VMEM((STEPS, 2, 5, 3, 8, 128), f32),
            pltpu.VMEM((STEPS, 5, 4, 3, 8, 128), f32),
            pltpu.VMEM((STEPS, 5, 3, 8, 128), f32),
            pltpu.VMEM((STEPS, 4, 3, 8, 128), f32),
            pltpu.VMEM((STEPS, 4, 3, 8, 128), f32),
            pltpu.VMEM((5, 8, 128), i32),
            pltpu.VMEM((5, 8, 128), i32),
            pltpu.VMEM((5, 8, 128), i32),
            pltpu.SMEM((5, 8, 128), i32),
            pltpu.VMEM((16, slots), f32),
            pltpu.VMEM((9 * SR, 128), f32),
            pltpu.VMEM((9 * SR, 128), f32),
            pltpu.VMEM((30, 128, KR), bf16),
            pltpu.VMEM((150, KR, 128), bf16),
            pltpu.VMEM((30, 16, 128), bf16),
            pltpu.VMEM((150, 16, 128), bf16),
            pltpu.VMEM((2, NB, 128, 128), f32),
            pltpu.VMEM((2, NB, 2, 128, 128), bf16),
            pltpu.VMEM((9 * SLOTS, 128), f32),
            pltpu.VMEM((9 * SLOTS, 128), f32),
            pltpu.VMEM((200, 2 * SLOTS), bf16),
            pltpu.VMEM((40, 2 * SLOTS), bf16),
            pltpu.SemaphoreType.DMA((5,)),
            pltpu.SemaphoreType.DMA((5,)),
            pltpu.SemaphoreType.DMA((STEPS, 63)),
            pltpu.SemaphoreType.DMA((STEPS, 63)),
        ],
        compiler_params=pltpu.CompilerParams(collective_id=0, has_side_effects=True),
        name="leapfrog",
    )(pairs, x, v, q, atoms)
    return tuple(out.reshape(positions.shape) for out in outs)


def solution(mesh):
    spec3 = P(None, "gx", "gy", "gz", None)
    spec1 = P("gx", "gy", "gz", None)
    sizes = tuple(mesh.shape[axis] for axis in AXES)
    return jax.shard_map(
        functools.partial(shards, sizes),
        mesh=mesh,
        in_specs=(spec3, spec3, spec1, spec1, spec3),
        out_specs=(spec3, spec3, spec3),
        check_vma=False,
    )
```
